32 devices in a mesh: blk: 16 (over z, x, core), tp: 2 (over y).
Axes of the slice: x: 2, y: 2, z: 4, core: 2. Of those that a mesh axis runs over, the one named last changes fastest.
Arguments:
- weights: float32 [16, 1024, 1024], P('blk', None, 'tp'), may hold values from -6 to 6
- copies: bfloat16 [16, 1024, 1024], P('blk', None, 'tp'), may hold values from -60 to 60
- copies_mixed: bfloat16 [16, 1024, 1024], P('blk', None, 'tp'), may hold values from -64 to 64
- tracker: bfloat16 [16, 1024, 1024], P('blk', None, 'tp'), may hold values from -6 to 6
- tracker_copy: bfloat16 [16, 1024, 1024], P('blk', None, 'tp'), may hold values from -6 to 6
- tracker_mixed: bfloat16 [16, 1024, 1024], P('blk', None, 'tp'), may hold values from -6 to 6
- grad_prev: bfloat16 [16, 1024, 1024], P('blk', None, 'tp'), may hold values from -3 to 3
- tokens: bfloat16 [16, 1024, 1024], P('blk', 'tp'), may hold values from -12 to 12
- image_ids: int32 [16, 1024], P('blk'), may hold values from 0 to 5, never falling along the last dimension, each value on 1 to 197 neighbouring positions
- key_weight: bfloat16 [1024, 1024], P(None, 'tp'), may hold values from -0.1875 to 0.1875
- value_weight: bfloat16 [1024, 1024], P(None, 'tp'), may hold values from -0.1875 to 0.1875
- out_grad: bfloat16 [16, 1024, 1024], P('blk', None, 'tp'), may hold values from -48 to 48
- row_picks: int32 [16, 2, 64], replicated, may hold values from 0 to 1023, as said below
Outputs:
- weights_new: float32 [16, 1024, 1024], P('blk', None, 'tp')
- copies_new: bfloat16 [16, 1024, 1024], P('blk', None, 'tp')
- mixed_new: bfloat16 [16, 1024, 1024], P('blk', None, 'tp')
- tracker_new: bfloat16 [16, 1024, 1024], P('blk', None, 'tp')
- tracker_copy_new: bfloat16 [16, 1024, 1024], P('blk', None, 'tp')
- tracker_mixed_new: bfloat16 [16, 1024, 1024], P('blk', None, 'tp')
- grad_new: bfloat16 [16, 1024, 1024], P('blk', None, 'tp')
- consensus: float32 [], replicated
The draws below stay inside these ranges and needn't reach their ends.
Inputs may be any that keep to these rules, and one draw needn't show every extreme that they name: `image_ids`: never falling along a replica's tokens; an image holds 1 to 197 tokens. `row_picks`: each row lists 64 different rows; the same picks serve every head shard of a replica.
All inputs are finite; a program needn't handle non-finite values.
Results may differ from the reference program's by a relative error of at most 0.0095.
The reference program's roundings to bfloat16 on the way (of `query_weight`, `score_grad` and `query_grad`) count: a program that leaves them out, or rounds other values in their place, can miss the bound.
Values may be sent and summed in bfloat16 or wider, within the bound.
A program may use at most 128 MiB of HBM per device.

```python
import math
import jax
import jax.numpy as jnp
import numpy as np
from jax import lax

D = 1024
HEADS = 16
HD = 64
SEG_MOST = 197
ROWS = 1024
KBLK = 64
IMGS = 6
N_BLK = 16


def key_matrix(key):
    noise_key = jax.random.fold_in(key, 7002)
    base = jnp.clip(jax.random.normal(noise_key, (D, D), jnp.float32), -6.0, 6.0)
    return (base * D ** (-0.5)).astype(jnp.bfloat16)


def draw_key_weight(key, part):
    return key_matrix(key)


def draw_weights(key, part):
    own_key = jax.random.fold_in(key, 7003)
    full_shape = (N_BLK, D, D)
    return jnp.clip(jax.random.normal(own_key, full_shape, jnp.float32), -6.0, 6.0)


def draw_tokens(key, part):
    own_key = jax.random.fold_in(key, 7004)
    normal_key = jax.random.fold_in(own_key, 0)
    full_shape = (N_BLK, ROWS, D)
    values = jax.random.normal(normal_key, full_shape, jnp.float32)
    return jnp.clip(values, -6.0, 6.0).astype(jnp.bfloat16)


def copy_fields(key):
    base_key = jax.random.fold_in(key, 7010)
    keys_all = jax.random.split(base_key, 8)
    full_shape = (N_BLK, D, D)
    replica = jnp.arange(N_BLK, dtype=jnp.float32)
    level = (1.0 + 2.0 * replica / max(N_BLK - 1, 1)) * jnp.exp(jax.random.uniform(keys_all[0], (N_BLK,), jnp.float32) * jnp.log(1.5))
    column = jnp.arange(D, dtype=jnp.float32) / max(D - 1, 1)
    group_count = D // 16
    rise_groups = jnp.repeat(jnp.exp(jax.random.uniform(keys_all[2], (group_count,), jnp.float32) * jnp.log(2.0)), 16)
    fall_groups = jnp.repeat(jnp.exp(jax.random.uniform(keys_all[3], (group_count,), jnp.float32) * jnp.log(2.0)), 16)
    rising = jnp.exp(jnp.log(6.0) * column) * rise_groups
    falling = jnp.exp(jnp.log(6.0) * (1.0 - column)) * fall_groups
    copy_rows = jnp.exp(jax.random.uniform(keys_all[4], (N_BLK, D, 1), jnp.float32) * jnp.log(3.0))
    gap_rows = jnp.exp(jax.random.uniform(keys_all[5], (N_BLK, D, 1), jnp.float32) * jnp.log(3.0))
    copy_noise = jnp.clip(jax.random.normal(keys_all[6], full_shape, jnp.float32), -4.0, 4.0)
    gap_noise = jnp.clip(jax.random.normal(keys_all[7], full_shape, jnp.float32), -4.0, 4.0)
    copies_value = jnp.clip(0.15 * level[:, None, None] * copy_rows * rising[None, None, :] * copy_noise, -60.0, 60.0)
    gap_value = 0.02 * level[:, None, None] * gap_rows * falling[None, None, :] * gap_noise
    mixed_value = jnp.clip(copies_value + gap_value, -64.0, 64.0)
    return (copies_value, mixed_value)


def draw_copies(key, part):
    copies_value, mixed_value = copy_fields(key)
    return copies_value.astype(jnp.bfloat16)


def draw_copies_mixed(key, part):
    copies_value, mixed_value = copy_fields(key)
    return mixed_value.astype(jnp.bfloat16)


def draw_row_picks(key, part):
    own_key = jax.random.fold_in(key, 7006)
    keys_all = jax.random.split(own_key, N_BLK * 2)
    picked = jax.vmap(lambda single: jax.random.permutation(single, D)[:KBLK])(keys_all)
    return picked.reshape(N_BLK, 2, KBLK).astype(jnp.int32)


def shard_levels(rng, extent, pieces, least, largest):
    def one(dim, parts):
        draws = jax.random.uniform(jax.random.fold_in(jax.random.fold_in(rng, 6), dim), (parts,), jnp.float32, least / len(pieces), largest / len(pieces))
        return jnp.repeat(jnp.exp(draws), extent[dim] // parts).reshape((-1,) + (1,) * (len(extent) - dim - 1))

    factor_of = one(*pieces[0])
    for cut in pieces[1:]:
        factor_of = factor_of * one(*cut)
    return factor_of


def length_profile(amount, total, reach, slope):
    portions = [(1 << 20) // math.isqrt(grade ** slope) + 1 for grade in range(2, amount + 1)]
    surplus, counts = total - reach - (amount - 1), [1] * (amount - 1)
    while surplus > 0:
        free = [i for i in range(amount - 1) if counts[i] < reach]
        mass, remaining = sum([portions[i] for i in free]), surplus
        for i in free:
            extra = min(reach - counts[i], max(1, remaining * portions[i] // mass), surplus)
            counts[i] = counts[i] + extra
            surplus = surplus - extra
    return np.array([reach] + counts)


def ragged(key, number_of, total, bound, slope):
    if number_of == 2:
        one = jax.random.randint(key, (), max(1, total - bound), min(bound, total - 1) + 1)
        return jnp.stack([one, total - one])
    lengths = jnp.asarray(length_profile(number_of, total, bound, slope), jnp.int32)
    twos = (number_of - 1) // 2
    giver, taker = lengths[1:1 + 2 * twos:2], lengths[2:2 + 2 * twos:2]
    margin = jnp.minimum(giver - 1, bound - taker)
    passed = jax.random.randint(jax.random.fold_in(key, 1), (twos,), 0, 1 << 20) % (margin + 1)
    lengths = lengths.at[1:1 + 2 * twos:2].set(giver - passed).at[2:2 + 2 * twos:2].set(taker + passed)
    return lengths[jax.random.permutation(jax.random.fold_in(key, 2), number_of)]


def normal_values(key, extent, scale, reach, pieces=(), held_as=jnp.bfloat16):
    gain = shard_levels(key, extent, pieces, -0.22, 0.18) if pieces else 1.0
    result = jax.random.normal(key, extent, jnp.float32) * scale * gain
    return jnp.minimum(jnp.maximum(result, -reach), reach).astype(held_as)


def setup_inputs(seed: int = 0) -> dict:
    key_list = jax.random.split(jax.random.key(seed), 14)
    weights = draw_weights(jax.random.fold_in(key_list[13], 71), 0)
    copies = draw_copies(jax.random.fold_in(key_list[13], 71), 0)
    copies_mixed = draw_copies_mixed(jax.random.fold_in(key_list[13], 71), 0)
    tracker = normal_values(key_list[3], (N_BLK, D, D), 1.0, 6.0, ((0, 16), (2, 2)))
    tracker_copy = normal_values(key_list[4], (N_BLK, D, D), 1.0, 6.0, ((0, 16), (2, 2)))
    tracker_mixed = normal_values(key_list[5], (N_BLK, D, D), 1.0, 6.0, ((0, 16), (2, 2)))
    grad_prev = normal_values(key_list[6], (N_BLK, D, D), 0.5, 3.0, ((0, 16), (2, 2)))
    tokens = draw_tokens(jax.random.fold_in(key_list[13], 71), 0)
    image_ids = jax.vmap(lambda own: jnp.searchsorted(jnp.cumsum(ragged(own, IMGS, ROWS, SEG_MOST, 0)), jnp.arange(ROWS), side="right"))(jax.random.split(key_list[8], N_BLK)).reshape((N_BLK, ROWS)).astype(jnp.int32)
    key_weight = draw_key_weight(jax.random.fold_in(key_list[13], 71), 0)
    value_weight = normal_values(key_list[10], (D, D), D ** -0.5, 0.1875, ((1, 2),))
    out_grad = normal_values(key_list[11], (N_BLK, ROWS, D), 8.0, 48.0, ((0, 16), (2, 2)))
    row_picks = draw_row_picks(jax.random.fold_in(key_list[13], 71), 0)
    return dict(weights=weights, copies=copies, copies_mixed=copies_mixed, tracker=tracker, tracker_copy=tracker_copy, tracker_mixed=tracker_mixed, grad_prev=grad_prev, tokens=tokens, image_ids=image_ids, key_weight=key_weight, value_weight=value_weight, out_grad=out_grad, row_picks=row_picks)


mixing_rate = 0.2
step_rate = 0.5

def contract(left, right, left_dim, right_dim):
    return lax.dot_general(left.astype(jnp.float32), right.astype(jnp.float32), (((left_dim,), (right_dim,)), ((), ())), preferred_element_type=jnp.float32)

def pick_matrix(picks):
    columns = jnp.arange(D, dtype=jnp.int32)
    return (picks[:, None] == columns[None, :]).astype(jnp.float32)

def compress(picks, field):
    matrix = pick_matrix(picks)
    kept = jnp.dot(matrix, field, precision=lax.Precision.HIGHEST)
    return jnp.dot(matrix.T, kept, precision=lax.Precision.HIGHEST)

def gossip_mix(update):
    return (jnp.roll(update, 1, axis=0) + update + jnp.roll(update, -1, axis=0)) / 3.0

def head_grad(query_head, key_head, value_head, out_head, same_image):
    scores = contract(query_head, key_head, 1, 1) * HD ** (-0.5)
    scores = jnp.where(same_image, scores, -1e+30)
    row_max = lax.optimization_barrier(jnp.max(scores, axis=-1, keepdims=True))
    exponent = jnp.exp(scores - row_max)
    attention = exponent / lax.optimization_barrier(jnp.sum(exponent, axis=-1, keepdims=True))
    out_proj = contract(out_head, value_head, 1, 1)
    centred = out_proj - lax.optimization_barrier(jnp.sum(attention * out_proj, axis=-1, keepdims=True))
    score_grad = (attention * centred * HD ** (-0.5)).astype(jnp.bfloat16)
    return jnp.dot(score_grad.astype(jnp.float32), key_head.astype(jnp.float32), preferred_element_type=jnp.float32).astype(jnp.bfloat16)

def replica_grad(weights_row, token_rows, image_row, out_rows, key_weight, value_weight):
    query_weight = (weights_row * D ** (-0.5)).astype(jnp.bfloat16)
    queries = jnp.dot(token_rows.astype(jnp.float32), query_weight.astype(jnp.float32), preferred_element_type=jnp.float32).astype(jnp.bfloat16)
    keyed = jnp.dot(token_rows.astype(jnp.float32), key_weight.astype(jnp.float32), preferred_element_type=jnp.float32).astype(jnp.bfloat16)
    valued = jnp.dot(token_rows.astype(jnp.float32), value_weight.astype(jnp.float32), preferred_element_type=jnp.float32).astype(jnp.bfloat16)
    same_image = image_row[:, None] == image_row[None, :]
    pieces_list = []
    for head_index in range(HEADS):
        low_col = head_index * HD
        pieces_list.append(head_grad(queries[:, low_col:low_col + HD], keyed[:, low_col:low_col + HD], valued[:, low_col:low_col + HD], out_rows[:, low_col:low_col + HD], same_image))
    query_grad = jnp.concatenate(pieces_list, axis=1)
    return (contract(token_rows, query_grad, 0, 0) * D ** (-0.5)).astype(jnp.bfloat16)

def reference(weights, copies, copies_mixed, tracker, tracker_copy, tracker_mixed, grad_prev, tokens, image_ids, key_weight, value_weight, out_grad, row_picks):
    copy_value = copies.astype(jnp.float32)
    weights_new = weights + mixing_rate * (copies_mixed.astype(jnp.float32) - copy_value) - step_rate * tracker.astype(jnp.float32)
    param_update = jax.vmap(compress)(row_picks[:, 0], weights_new - copy_value)
    copies_new = (copy_value + param_update).astype(jnp.bfloat16)
    mixed_new = (copies_mixed.astype(jnp.float32) + gossip_mix(param_update)).astype(jnp.bfloat16)

    def one_replica(packed):
        return replica_grad(packed[0], packed[1], packed[2], packed[3], key_weight, value_weight)
    grad_new = lax.map(one_replica, (weights_new, tokens, image_ids, out_grad))
    tracker_copy_value = tracker_copy.astype(jnp.float32)
    tracker_new = (tracker.astype(jnp.float32) + mixing_rate * (tracker_mixed.astype(jnp.float32) - tracker_copy_value) + grad_new.astype(jnp.float32) - grad_prev.astype(jnp.float32)).astype(jnp.bfloat16)
    tracker_update = jax.vmap(compress)(row_picks[:, 1], tracker_new.astype(jnp.float32) - tracker_copy_value)
    tracker_copy_new = (tracker_copy_value + tracker_update).astype(jnp.bfloat16)
    tracker_mixed_new = (tracker_mixed.astype(jnp.float32) + gossip_mix(tracker_update)).astype(jnp.bfloat16)
    gap_value = mixed_new.astype(jnp.float32) - copies_new.astype(jnp.float32)
    consensus = jnp.sum(gap_value * gap_value) / (N_BLK * D * D)
    return (weights_new, copies_new, mixed_new, tracker_new, tracker_copy_new, tracker_mixed_new, grad_new, consensus)
```

```python
import functools

import jax
import jax.numpy as jnp
from jax import lax
from jax.experimental import pallas as pl
from jax.experimental.pallas import tpu as pltpu
from jax.sharding import PartitionSpec as P

HD = 64
SEG_MOST = 197
TILE = 128

mixing_rate = 0.2
step_rate = 0.5

ANY = pl.BlockSpec(memory_space=pl.ANY)
VMEM = pl.BlockSpec(memory_space=pltpu.VMEM)


def contract(left, right, left_dim, right_dim):
    return lax.dot_general(
        left, right, (((left_dim,), (right_dim,)), ((), ())), preferred_element_type=jnp.float32
    )


def one_hot(picks, total_rows):
    columns = lax.broadcasted_iota(jnp.int32, (picks.shape[0], total_rows), 1)
    return (picks[:, None] == columns).astype(jnp.bfloat16)


def picked_rows(picks, total_rows):
    rows = lax.broadcasted_iota(jnp.int32, (total_rows, picks.shape[0]), 0)
    return jnp.any(rows == picks[None, :], axis=1, keepdims=True)


def replica_picks(row_picks, offset):
    count = lax.axis_size("blk")
    rank = lax.rem(lax.axis_index("blk") + offset + count, count)
    return lax.dynamic_index_in_dim(row_picks, rank, 0, keepdims=False)


def mix_stream(pieces, row_picks, stream, total_rows):
    picks = jnp.concatenate([replica_picks(row_picks, o)[stream] for o in (-1, 0, 1)], axis=0)
    values = jnp.concatenate(pieces, axis=0)
    return contract(one_hot(picks, total_rows), values, 0, 0) / 3.0


def gossip_kernel(
    blk_count, tp_count, values, part, lower, upper, total, slots, send_sem, recv_sem, part_sems
):
    blk, tp = lax.axis_index("blk"), lax.axis_index("tp")
    count = blk_count * tp_count
    me = blk * tp_count + tp
    mesh_type = pl.DeviceIdType.MESH
    barrier = pltpu.get_barrier_semaphore()

    def device(distance):
        flat = lax.rem(me + distance, count)
        return (flat // tp_count, lax.rem(flat, tp_count))

    def greet(distance, carry):
        pl.semaphore_signal(barrier, inc=1, device_id=device(distance), device_id_type=mesh_type)
        return carry

    lax.fori_loop(1, count, greet, 0)
    pl.semaphore_wait(barrier, count - 1)
    after = lax.rem(blk + 1, blk_count)
    before = lax.rem(blk + blk_count - 1, blk_count)
    up = pltpu.make_async_remote_copy(
        values, lower, send_sem.at[0], recv_sem.at[0], device_id=(after, tp), device_id_type=mesh_type
    )
    down = pltpu.make_async_remote_copy(
        values, upper, send_sem.at[1], recv_sem.at[1], device_id=(before, tp), device_id_type=mesh_type
    )
    up.start()
    down.start()

    def send(distance, carry):
        pltpu.make_async_remote_copy(
            part,
            slots.at[distance - 1],
            part_sems.at[0],
            part_sems.at[1],
            device_id=device(distance),
            device_id_type=mesh_type,
        ).start()
        return carry

    lax.fori_loop(1, count, send, 0)
    pltpu.make_async_copy(slots, slots, part_sems.at[1]).wait()
    pltpu.make_async_copy(slots, slots, part_sems.at[0]).wait()
    total[...] = jnp.sum(slots[...], axis=0) + part[...]
    up.wait()
    down.wait()


def gossip(values, part):
    blk_count, tp_count = lax.axis_size("blk"), lax.axis_size("tp")
    same = jax.ShapeDtypeStruct(values.shape, values.dtype)
    return pl.pallas_call(
        functools.partial(gossip_kernel, blk_count, tp_count),
        out_shape=(same, same, jax.ShapeDtypeStruct(part.shape, part.dtype)),
        in_specs=[VMEM, VMEM],
        out_specs=(VMEM, VMEM, VMEM),
        scratch_shapes=[
            pltpu.VMEM((blk_count * tp_count - 1,) + part.shape, part.dtype),
            pltpu.SemaphoreType.DMA((2,)),
            pltpu.SemaphoreType.DMA((2,)),
            pltpu.SemaphoreType.DMA((2,)),
        ],
        compiler_params=pltpu.CompilerParams(collective_id=0, has_side_effects=True),
        cost_estimate=pl.CostEstimate(flops=10000, bytes_accessed=10000000, transcendentals=0),
    )(values, part)


def gradient_kernel(count, *refs):
    pieces = refs[:count]
    (query_w, key_w, value_w, out_grad, ids_col, ids_row, picks_row, picks_col) = refs[count : count + 8]
    fields = refs[count + 8 : count + 12]
    grad_out, tracker_out, copy_out, kept = refs[count + 12 : count + 16]
    scratch = refs[count + 16 :]
    tok, qw, kw, vw, og, tr, tm, tc, gp, qs, ks, vs, qg, upd, bias, go, to, co, tok_sems, sems, out_sems = scratch
    total_rows, model_width = tok.shape
    width = qw.shape[1]
    rows_local = total_rows // count
    rank = lax.axis_index("tp")

    loads = []
    for shift in range(count):
        owner = lax.rem(rank - shift + count, count)
        where = pl.ds(pl.multiple_of(owner * rows_local, rows_local), rows_local)
        loads.append(pltpu.make_async_copy(pieces[shift], tok.at[where], tok_sems.at[shift]))
    sources = (query_w, key_w, value_w, out_grad) + fields
    for index, (source, target) in enumerate(zip(sources, (qw, kw, vw, og, tr, tm, tc, gp))):
        loads.append(pltpu.make_async_copy(source, target, sems.at[index]))
    for load in loads:
        load.start()
    for load in loads[: count + 3]:
        load.wait()

    proj = 256

    @pl.loop(0, total_rows // proj)
    def _(step):
        rows = pl.ds(pl.multiple_of(step * proj, proj), proj)
        block = tok[rows, :]
        query = jnp.dot(block, qw[...], preferred_element_type=jnp.float32).astype(jnp.bfloat16)
        qs[rows, :] = (query.astype(jnp.float32) * HD ** (-0.5)).astype(jnp.bfloat16)
        ks[rows, :] = jnp.dot(block, kw[...], preferred_element_type=jnp.float32).astype(jnp.bfloat16)
        vs[rows, :] = jnp.dot(block, vw[...], preferred_element_type=jnp.float32).astype(jnp.bfloat16)

    loads[count + 3].wait()
    pair = 2 * HD
    lane = lax.broadcasted_iota(jnp.int32, (1, pair), 1)
    first = jnp.where(lane < HD, 1.0, 0.0).astype(jnp.bfloat16)
    second = jnp.where(lane < HD, 0.0, 1.0).astype(jnp.bfloat16)
    reach = SEG_MOST - 1
    for low in range(0, total_rows, TILE):
        start = max(0, (low - reach) // TILE * TILE)
        end = min(total_rows, -(-(low + TILE + reach) // TILE) * TILE)
        span = end - start
        same = ids_col[low : low + TILE, :] == ids_row[:, start:end]
        tile_bias = jnp.where(same, 0.0, -1e30)
        bias[:TILE, :span] = tile_bias
        bias[TILE:, :span] = tile_bias

        @pl.loop(0, width // pair)
        def _(index):
            columns = pl.ds(pl.multiple_of(index * pair, pair), pair)
            query = qs[low : low + TILE, columns]
            outer = og[low : low + TILE, columns]
            keyed = ks[start:end, columns]
            valued = vs[start:end, columns]
            queries = jnp.concatenate([query * first, query * second], axis=0)
            outers = jnp.concatenate([outer * first, outer * second], axis=0)
            scores = contract(queries, keyed, 1, 1) + bias[:, :span]
            out_proj = contract(outers, valued, 1, 1)
            exponent = jnp.exp(scores - jnp.max(scores, axis=-1, keepdims=True))
            inverse = 1.0 / jnp.sum(exponent, axis=-1, keepdims=True)
            centre = jnp.sum(exponent * out_proj, axis=-1, keepdims=True) * inverse
            score_grad = (exponent * ((out_proj - centre) * (inverse * HD ** (-0.5)))).astype(
                jnp.bfloat16
            )
            both = jnp.dot(score_grad, keyed, preferred_element_type=jnp.float32)
            qg[low : low + TILE, columns] = jnp.where(lane < HD, both[:TILE], both[TILE:]).astype(
                jnp.bfloat16
            )

    for load in loads[count + 4 :]:
        load.wait()

    @pl.loop(0, model_width // TILE)
    def _(step):
        base = pl.multiple_of(step * TILE, TILE)
        rows = pl.ds(base, TILE)
        product = contract(tok[:, rows], qg[...], 0, 0)
        grad = (product * model_width ** (-0.5)).astype(jnp.bfloat16)
        copy = tc[rows, :].astype(jnp.float32)
        new = (
            tr[rows, :].astype(jnp.float32)
            + mixing_rate * (tm[rows, :].astype(jnp.float32) - copy)
            + grad.astype(jnp.float32)
            - gp[rows, :].astype(jnp.float32)
        ).astype(jnp.bfloat16)
        change = new.astype(jnp.float32) - copy
        index = lax.broadcasted_iota(jnp.int32, (TILE, picks_row.shape[1]), 0) + base
        hits = jnp.where(index == picks_row[...], 1.0, 0.0)
        picked = jnp.max(hits, axis=1, keepdims=True)
        go[rows, :] = grad
        to[rows, :] = new
        co[rows, :] = (copy + change * picked).astype(jnp.bfloat16)
        upd[rows, :] = change.astype(jnp.bfloat16)
        for slot, (source, target) in enumerate(((go, grad_out), (to, tracker_out), (co, copy_out))):
            pltpu.make_async_copy(source.at[rows], target.at[rows], out_sems.at[slot]).start()

    columns = lax.broadcasted_iota(jnp.int32, (picks_col.shape[0], model_width), 1)
    matrix = jnp.where(picks_col[...] == columns, 1.0, 0.0).astype(jnp.bfloat16)
    kept[...] = jnp.dot(matrix, upd[...], preferred_element_type=jnp.float32).astype(jnp.bfloat16)
    for slot, (source, target) in enumerate(((go, grad_out), (to, tracker_out), (co, copy_out))):
        pltpu.make_async_copy(source, target, out_sems.at[slot]).wait()


def gradient_stage(pieces, query_weight, key_weight, value_weight, out_grad, image_row, picks, fields):
    count = len(pieces)
    rows_local, model_width = pieces[0].shape
    total_rows = rows_local * count
    width = query_weight.shape[1]
    bf16 = jnp.bfloat16
    field = jax.ShapeDtypeStruct((model_width, width), bf16)
    span_most = min(total_rows, TILE + 2 * (-(-(SEG_MOST - 1) // TILE) * TILE))
    weight = pltpu.VMEM((model_width, width), bf16)
    row_block = pltpu.VMEM((total_rows, width), bf16)
    return pl.pallas_call(
        functools.partial(gradient_kernel, count),
        out_shape=(field, field, field, jax.ShapeDtypeStruct((picks.shape[0], width), bf16)),
        in_specs=[ANY] * (count + 4) + [VMEM] * 4 + [ANY] * 4,
        out_specs=(ANY, ANY, ANY, VMEM),
        scratch_shapes=[pltpu.VMEM((total_rows, model_width), bf16)]
        + [weight] * 3
        + [row_block]
        + [weight] * 4
        + [row_block] * 4
        + [weight, pltpu.VMEM((2 * TILE, span_most), jnp.float32)]
        + [weight] * 3
        + [
            pltpu.SemaphoreType.DMA((count,)),
            pltpu.SemaphoreType.DMA((8,)),
            pltpu.SemaphoreType.DMA((3,)),
        ],
        compiler_params=pltpu.CompilerParams(vmem_limit_bytes=56 * 2**20),
        cost_estimate=pl.CostEstimate(
            flops=8 * total_rows * model_width * width + 6 * total_rows * 640 * width,
            bytes_accessed=24 * model_width * width,
            transcendentals=total_rows * 640 * width // HD,
        ),
    )(
        *pieces,
        query_weight,
        key_weight,
        value_weight,
        out_grad,
        image_row.reshape(total_rows, 1),
        image_row.reshape(1, total_rows),
        picks.reshape(1, -1),
        picks.reshape(-1, 1),
        *fields,
    )


def per_device(
    weights,
    copies,
    copies_mixed,
    tracker,
    tracker_copy,
    tracker_mixed,
    grad_prev,
    tokens,
    image_ids,
    key_weight,
    value_weight,
    out_grad,
    row_picks,
):
    model_width = weights.shape[1]
    blk_count, tp_count = lax.axis_size("blk"), lax.axis_size("tp")
    pieces = [tokens[0]]
    for shift in range(1, tp_count):
        pieces.append(
            lax.ppermute(tokens[0], "tp", [(i, (i + shift) % tp_count) for i in range(tp_count)])
        )
    own_picks = replica_picks(row_picks, 0)
    copy_value = copies[0].astype(jnp.float32)
    mixed_value = copies_mixed[0].astype(jnp.float32)
    weights_new = (
        weights[0]
        + mixing_rate * (mixed_value - copy_value)
        - step_rate * tracker[0].astype(jnp.float32)
    )
    query_weight = (weights_new * model_width ** (-0.5)).astype(jnp.bfloat16)
    update = weights_new - copy_value
    picked = picked_rows(own_picks[0], model_width)
    copies_new = jnp.where(picked, copy_value + update, copy_value).astype(jnp.bfloat16)
    kept = contract(
        one_hot(own_picks[0], model_width), update.astype(jnp.bfloat16), 1, 0
    ).astype(jnp.bfloat16)
    up = [(i, (i + 1) % blk_count) for i in range(blk_count)]
    down = [(j, i) for i, j in up]
    lower = lax.ppermute(kept, "blk", up)
    upper = lax.ppermute(kept, "blk", down)
    mixed_new = (
        mixed_value + mix_stream([lower, kept, upper], row_picks, 0, model_width)
    ).astype(jnp.bfloat16)
    gap = mixed_new.astype(jnp.float32) - copies_new.astype(jnp.float32)
    part = jnp.broadcast_to(jnp.sum(gap * gap)[None, None], (8, 128))

    grad_new, tracker_new, tracker_copy_new, kept = gradient_stage(
        pieces,
        query_weight,
        key_weight,
        value_weight,
        out_grad[0],
        image_ids[0],
        own_picks[1],
        (tracker[0], tracker_mixed[0], tracker_copy[0], grad_prev[0]),
    )
    lower, upper, total = gossip(kept, part)
    tracker_mixed_new = (
        tracker_mixed[0].astype(jnp.float32)
        + mix_stream([lower, kept, upper], row_picks, 1, model_width)
    ).astype(jnp.bfloat16)
    entries = float(blk_count * model_width * model_width)
    return (
        weights_new[None],
        copies_new[None],
        mixed_new[None],
        tracker_new[None],
        tracker_copy_new[None],
        tracker_mixed_new[None],
        grad_new[None],
        total[0, 0] / entries,
    )


def solution(mesh):
    field = P("blk", None, "tp")
    return jax.shard_map(
        per_device,
        mesh=mesh,
        in_specs=(field,) * 7
        + (P("blk", "tp", None), P("blk", None), P(None, "tp"), P(None, "tp"), field, P()),
        out_specs=(field,) * 7 + (P(),),
        check_vma=False,
    )
```

```python
import functools

import jax
import jax.numpy as jnp
from jax import lax
from jax.experimental import pallas as pl
from jax.experimental.pallas import tpu as pltpu
from jax.sharding import PartitionSpec as P

HD = 64
SEG_MOST = 197
TILE = 128

mixing_rate = 0.2
step_rate = 0.5

ANY = pl.BlockSpec(memory_space=pl.ANY)
VMEM = pl.BlockSpec(memory_space=pltpu.VMEM)


def contract(left, right, left_dim, right_dim):
    return lax.dot_general(
        left, right, (((left_dim,), (right_dim,)), ((), ())), preferred_element_type=jnp.float32
    )


def one_hot(picks, total_rows):
    columns = lax.broadcasted_iota(jnp.int32, (picks.shape[0], total_rows), 1)
    return (picks[:, None] == columns).astype(jnp.bfloat16)


def picked_rows(picks, total_rows):
    rows = lax.broadcasted_iota(jnp.int32, (total_rows, picks.shape[0]), 0)
    return jnp.any(rows == picks[None, :], axis=1, keepdims=True)


def replica_picks(row_picks, offset):
    count = lax.axis_size("blk")
    rank = lax.rem(lax.axis_index("blk") + offset + count, count)
    return lax.dynamic_index_in_dim(row_picks, rank, 0, keepdims=False)


def mix_stream(pieces, row_picks, stream, total_rows):
    picks = jnp.concatenate([replica_picks(row_picks, o)[stream] for o in (-1, 0, 1)], axis=0)
    values = jnp.concatenate(pieces, axis=0)
    return contract(one_hot(picks, total_rows), values, 0, 0) / 3.0


def gossip_kernel(
    blk_count, tp_count, values, part, lower, upper, total, slots, send_sem, recv_sem, part_sems
):
    blk, tp = lax.axis_index("blk"), lax.axis_index("tp")
    count = blk_count * tp_count
    me = blk * tp_count + tp
    mesh_type = pl.DeviceIdType.MESH
    barrier = pltpu.get_barrier_semaphore()

    def device(distance):
        flat = lax.rem(me + distance, count)
        return (flat // tp_count, lax.rem(flat, tp_count))

    def greet(distance, carry):
        pl.semaphore_signal(barrier, inc=1, device_id=device(distance), device_id_type=mesh_type)
        return carry

    lax.fori_loop(1, count, greet, 0)
    pl.semaphore_wait(barrier, count - 1)
    after = lax.rem(blk + 1, blk_count)
    before = lax.rem(blk + blk_count - 1, blk_count)
    up = pltpu.make_async_remote_copy(
        values, lower, send_sem.at[0], recv_sem.at[0], device_id=(after, tp), device_id_type=mesh_type
    )
    down = pltpu.make_async_remote_copy(
        values, upper, send_sem.at[1], recv_sem.at[1], device_id=(before, tp), device_id_type=mesh_type
    )
    up.start()
    down.start()

    def send(distance, carry):
        pltpu.make_async_remote_copy(
            part,
            slots.at[distance - 1],
            part_sems.at[0],
            part_sems.at[1],
            device_id=device(distance),
            device_id_type=mesh_type,
        ).start()
        return carry

    lax.fori_loop(1, count, send, 0)
    pltpu.make_async_copy(slots, slots, part_sems.at[1]).wait()
    pltpu.make_async_copy(slots, slots, part_sems.at[0]).wait()
    total[...] = jnp.sum(slots[...], axis=0) + part[...]
    up.wait()
    down.wait()


def gossip(values, part):
    blk_count, tp_count = lax.axis_size("blk"), lax.axis_size("tp")
    same = jax.ShapeDtypeStruct(values.shape, values.dtype)
    return pl.pallas_call(
        functools.partial(gossip_kernel, blk_count, tp_count),
        out_shape=(same, same, jax.ShapeDtypeStruct(part.shape, part.dtype)),
        in_specs=[VMEM, VMEM],
        out_specs=(VMEM, VMEM, VMEM),
        scratch_shapes=[
            pltpu.VMEM((blk_count * tp_count - 1,) + part.shape, part.dtype),
            pltpu.SemaphoreType.DMA((2,)),
            pltpu.SemaphoreType.DMA((2,)),
            pltpu.SemaphoreType.DMA((2,)),
        ],
        compiler_params=pltpu.CompilerParams(collective_id=0, has_side_effects=True),
        cost_estimate=pl.CostEstimate(flops=10000, bytes_accessed=10000000, transcendentals=0),
    )(values, part)


def attend(lows, total_rows, qs, ks, vs, og, qg, ids_col, ids_row, bias):
    width = qs.shape[1]
    pair = 2 * HD
    lane = lax.broadcasted_iota(jnp.int32, (1, pair), 1)
    first = jnp.where(lane < HD, 1.0, 0.0).astype(jnp.bfloat16)
    second = jnp.where(lane < HD, 0.0, 1.0).astype(jnp.bfloat16)
    reach = SEG_MOST - 1
    for low in lows:
        start = max(0, (low - reach) // TILE * TILE)
        end = min(total_rows, -(-(low + TILE + reach) // TILE) * TILE)
        span = end - start
        same = ids_col[low : low + TILE, :] == ids_row[:, start:end]
        tile_bias = jnp.where(same, 0.0, -1e30)
        bias[:TILE, :span] = tile_bias
        bias[TILE:, :span] = tile_bias

        @pl.loop(0, width // pair, unroll=2 if width // pair % 2 == 0 else 1)
        def _(index):
            columns = pl.ds(pl.multiple_of(index * pair, pair), pair)
            query = qs[low : low + TILE, columns]
            outer = og[low : low + TILE, columns]
            keyed = ks[start:end, columns]
            valued = vs[start:end, columns]
            queries = jnp.concatenate([query * first, query * second], axis=0)
            outers = jnp.concatenate([outer * first, outer * second], axis=0)
            scores = contract(queries, keyed, 1, 1) + bias[:, :span]
            out_proj = contract(outers, valued, 1, 1)
            exponent = jnp.exp(scores - jnp.max(scores, axis=-1, keepdims=True))
            inverse = 1.0 / jnp.sum(exponent, axis=-1, keepdims=True)
            centre = jnp.sum(exponent * out_proj, axis=-1, keepdims=True) * inverse
            score_grad = (exponent * ((out_proj - centre) * (inverse * HD ** (-0.5)))).astype(
                jnp.bfloat16
            )
            both = jnp.dot(score_grad, keyed, preferred_element_type=jnp.float32)
            qg[low : low + TILE, columns] = jnp.where(lane < HD, both[:TILE], both[TILE:]).astype(
                jnp.bfloat16
            )


def project(start, steps, tok, qw, kw, vw, qs, ks, vs, proj):
    @pl.loop(0, steps)
    def _(step):
        rows = pl.ds(pl.multiple_of(start + step * proj, proj), proj)
        block = tok[rows, :]
        query = jnp.dot(block, qw[...], preferred_element_type=jnp.float32).astype(jnp.bfloat16)
        qs[rows, :] = (query.astype(jnp.float32) * HD ** (-0.5)).astype(jnp.bfloat16)
        ks[rows, :] = jnp.dot(block, kw[...], preferred_element_type=jnp.float32).astype(jnp.bfloat16)
        vs[rows, :] = jnp.dot(block, vw[...], preferred_element_type=jnp.float32).astype(jnp.bfloat16)


def piece_rows(index, rank, local, split, count):
    if split:
        half = local // 2
        start = (rank * local, local - rank * half, (local + half) * (1 - rank))[index]
        return pl.ds(pl.multiple_of(start, half), local if index == 0 else half)
    start = lax.rem(rank - index + count, count) * local
    return pl.ds(pl.multiple_of(start, local), local)


def own_kernel(own, near, query_w, key_w, value_w, out_grad, ids_col, ids_row, done, *scratch):
    tok, qw, kw, vw, og, qs, ks, vs, qg, bias, sems = scratch
    total_rows = tok.shape[0]
    local = own.shape[0]
    half = local // 2
    rank = lax.axis_index("tp")
    own_rows = piece_rows(0, rank, local, True, 2)
    targets = (
        tok.at[own_rows],
        tok.at[piece_rows(1, rank, local, True, 2)],
        qw,
        kw,
        vw,
        og,
    )
    loads = [
        pltpu.make_async_copy(source, target, sems.at[index])
        for index, (source, target) in enumerate(
            zip((own, near, query_w, key_w, value_w, out_grad), targets)
        )
    ]
    for load in loads:
        load.start()
    for load in loads:
        load.wait()
    project(rank * half, 3, tok, qw, kw, vw, qs, ks, vs, half)
    for side in range(2):

        @pl.when(rank == side)
        def _():
            lows = range(side * local, (side + 1) * local, TILE)
            attend(lows, total_rows, qs, ks, vs, og, qg, ids_col, ids_row, bias)

    done[...] = qg[own_rows, :]


def own_stage(own, near, query_weight, key_weight, value_weight, out_grad, image_row):
    local, model_width = own.shape
    total_rows, width = out_grad.shape
    bf16 = jnp.bfloat16
    weight = pltpu.VMEM((model_width, width), bf16)
    row_block = pltpu.VMEM((total_rows, width), bf16)
    return pl.pallas_call(
        own_kernel,
        out_shape=jax.ShapeDtypeStruct((local, width), bf16),
        in_specs=[ANY] * 6 + [VMEM] * 2,
        out_specs=VMEM,
        scratch_shapes=[pltpu.VMEM((total_rows, model_width), bf16)]
        + [weight] * 3
        + [row_block] * 5
        + [pltpu.VMEM((2 * TILE, span_limit(total_rows)), jnp.float32)]
        + [pltpu.SemaphoreType.DMA((6,))],
        compiler_params=pltpu.CompilerParams(vmem_limit_bytes=40 * 2**20),
        cost_estimate=pl.CostEstimate(
            flops=4 * total_rows * model_width * width,
            bytes_accessed=12 * model_width * width,
            transcendentals=total_rows * 320 * width // HD,
        ),
    )(
        own,
        near,
        query_weight,
        key_weight,
        value_weight,
        out_grad,
        image_row.reshape(total_rows, 1),
        image_row.reshape(1, total_rows),
    )


def span_limit(total_rows):
    return min(total_rows, TILE + 2 * (-(-(SEG_MOST - 1) // TILE) * TILE))


def gradient_kernel(count, split, *refs):
    pieces = refs[:count]
    done, refs = (refs[count], refs[:count] + refs[count + 1 :]) if split else (None, refs)
    (query_w, key_w, value_w, out_grad, ids_col, ids_row, picks_row, picks_col) = refs[count : count + 8]
    fields = refs[count + 8 : count + 12]
    grad_out, tracker_out, copy_out, kept = refs[count + 12 : count + 16]
    scratch = refs[count + 16 :]
    tok, qw, kw, vw, og, tr, tm, tc, gp, qs, ks, vs, qg, upd, bias, go, to, co, tok_sems, sems, out_sems = scratch
    total_rows, model_width = tok.shape
    rank = lax.axis_index("tp")

    loads = []
    for shift in range(count):
        where = piece_rows(shift, rank, pieces[0].shape[0], split, count)
        loads.append(pltpu.make_async_copy(pieces[shift], tok.at[where], tok_sems.at[shift]))
    sources = (query_w, key_w, value_w, out_grad) + fields
    for index, (source, target) in enumerate(zip(sources, (qw, kw, vw, og, tr, tm, tc, gp))):
        loads.append(pltpu.make_async_copy(source, target, sems.at[index]))
    if split:
        own_rows = piece_rows(0, rank, pieces[0].shape[0], True, count)
        loads.append(pltpu.make_async_copy(done, qg.at[own_rows], sems.at[8]))
    for load in loads:
        load.start()
    for load in loads[: count + 4]:
        load.wait()

    project(0, total_rows // 256, tok, qw, kw, vw, qs, ks, vs, 256)
    if split:
        local = pieces[0].shape[0]
        for side in range(2):

            @pl.when(rank == side)
            def _():
                lows = range((1 - side) * local, (2 - side) * local, TILE)
                attend(lows, total_rows, qs, ks, vs, og, qg, ids_col, ids_row, bias)

    else:
        attend(range(0, total_rows, TILE), total_rows, qs, ks, vs, og, qg, ids_col, ids_row, bias)

    for load in loads[count + 4 :]:
        load.wait()

    @pl.loop(0, model_width // TILE)
    def _(step):
        base = pl.multiple_of(step * TILE, TILE)
        rows = pl.ds(base, TILE)
        product = contract(tok[:, rows], qg[...], 0, 0)
        grad = (product * model_width ** (-0.5)).astype(jnp.bfloat16)
        copy = tc[rows, :].astype(jnp.float32)
        new = (
            tr[rows, :].astype(jnp.float32)
            + mixing_rate * (tm[rows, :].astype(jnp.float32) - copy)
            + grad.astype(jnp.float32)
            - gp[rows, :].astype(jnp.float32)
        ).astype(jnp.bfloat16)
        change = new.astype(jnp.float32) - copy
        index = lax.broadcasted_iota(jnp.int32, (TILE, picks_row.shape[1]), 0) + base
        hits = jnp.where(index == picks_row[...], 1.0, 0.0)
        picked = jnp.max(hits, axis=1, keepdims=True)
        go[rows, :] = grad
        to[rows, :] = new
        co[rows, :] = (copy + change * picked).astype(jnp.bfloat16)
        upd[rows, :] = change.astype(jnp.bfloat16)
        for slot, (source, target) in enumerate(((go, grad_out), (to, tracker_out), (co, copy_out))):
            pltpu.make_async_copy(source.at[rows], target.at[rows], out_sems.at[slot]).start()

    columns = lax.broadcasted_iota(jnp.int32, (picks_col.shape[0], model_width), 1)
    matrix = jnp.where(picks_col[...] == columns, 1.0, 0.0).astype(jnp.bfloat16)
    kept[...] = jnp.dot(matrix, upd[...], preferred_element_type=jnp.float32).astype(jnp.bfloat16)
    for slot, (source, target) in enumerate(((go, grad_out), (to, tracker_out), (co, copy_out))):
        pltpu.make_async_copy(source, target, out_sems.at[slot]).wait()


def gradient_stage(pieces, done, query_weight, key_weight, value_weight, out_grad, image_row, picks, fields):
    count = len(pieces)
    model_width = pieces[0].shape[1]
    total_rows = out_grad.shape[0]
    extra = [] if done is None else [done]
    width = query_weight.shape[1]
    bf16 = jnp.bfloat16
    field = jax.ShapeDtypeStruct((model_width, width), bf16)
    weight = pltpu.VMEM((model_width, width), bf16)
    row_block = pltpu.VMEM((total_rows, width), bf16)
    return pl.pallas_call(
        functools.partial(gradient_kernel, count, done is not None),
        out_shape=(field, field, field, jax.ShapeDtypeStruct((picks.shape[0], width), bf16)),
        in_specs=[ANY] * (count + len(extra) + 4) + [VMEM] * 4 + [ANY] * 4,
        out_specs=(ANY, ANY, ANY, VMEM),
        scratch_shapes=[pltpu.VMEM((total_rows, model_width), bf16)]
        + [weight] * 3
        + [row_block]
        + [weight] * 4
        + [row_block] * 4
        + [weight, pltpu.VMEM((2 * TILE, span_limit(total_rows)), jnp.float32)]
        + [weight] * 3
        + [
            pltpu.SemaphoreType.DMA((count,)),
            pltpu.SemaphoreType.DMA((9,)),
            pltpu.SemaphoreType.DMA((3,)),
        ],
        compiler_params=pltpu.CompilerParams(vmem_limit_bytes=56 * 2**20),
        cost_estimate=pl.CostEstimate(
            flops=8 * total_rows * model_width * width + 6 * total_rows * 640 * width,
            bytes_accessed=24 * model_width * width,
            transcendentals=total_rows * 640 * width // HD,
        ),
    )(
        *pieces,
        *extra,
        query_weight,
        key_weight,
        value_weight,
        out_grad,
        image_row.reshape(total_rows, 1),
        image_row.reshape(1, total_rows),
        picks.reshape(1, -1),
        picks.reshape(-1, 1),
        *fields,
    )


def device_step(
    weights,
    copies,
    copies_mixed,
    tracker,
    tracker_copy,
    tracker_mixed,
    grad_prev,
    tokens,
    image_ids,
    key_weight,
    value_weight,
    out_grad,
    row_picks,
):
    model_width = weights.shape[1]
    blk_count, tp_count = lax.axis_size("blk"), lax.axis_size("tp")
    local = tokens.shape[1]
    half = local // 2
    split = tp_count == 2 and half % 256 == 0
    pieces = [tokens[0]]
    if split:
        rank = lax.axis_index("tp")
        swap = [(0, 1), (1, 0)]
        first = lax.dynamic_slice_in_dim(tokens[0], (1 - rank) * half, half, 0)
        pieces.append(lax.ppermute(first, "tp", swap))
        later = lax.dynamic_slice_in_dim(tokens[0], rank * half, half, 0)
        pieces.append(lax.ppermute(later, "tp", swap))
    else:
        for shift in range(1, tp_count):
            hop = [(i, (i + shift) % tp_count) for i in range(tp_count)]
            pieces.append(lax.ppermute(tokens[0], "tp", hop))
    own_picks = replica_picks(row_picks, 0)
    copy_value = copies[0].astype(jnp.float32)
    mixed_value = copies_mixed[0].astype(jnp.float32)
    weights_new = (
        weights[0]
        + mixing_rate * (mixed_value - copy_value)
        - step_rate * tracker[0].astype(jnp.float32)
    )
    query_weight = (weights_new * model_width ** (-0.5)).astype(jnp.bfloat16)
    update = weights_new - copy_value
    picked = picked_rows(own_picks[0], model_width)
    copies_new = jnp.where(picked, copy_value + update, copy_value).astype(jnp.bfloat16)
    kept = contract(
        one_hot(own_picks[0], model_width), update.astype(jnp.bfloat16), 1, 0
    ).astype(jnp.bfloat16)
    up = [(i, (i + 1) % blk_count) for i in range(blk_count)]
    down = [(j, i) for i, j in up]
    lower = lax.ppermute(kept, "blk", up)
    upper = lax.ppermute(kept, "blk", down)
    mixed_new = (
        mixed_value + mix_stream([lower, kept, upper], row_picks, 0, model_width)
    ).astype(jnp.bfloat16)
    gap = mixed_new.astype(jnp.float32) - copies_new.astype(jnp.float32)
    part = jnp.broadcast_to(jnp.sum(gap * gap)[None, None], (8, 128))

    part, query_weight = lax.optimization_barrier((part, query_weight))
    done = None
    if split:
        done = own_stage(
            pieces[0], pieces[1], query_weight, key_weight, value_weight, out_grad[0], image_ids[0]
        )
    grad_new, tracker_new, tracker_copy_new, kept = gradient_stage(
        pieces,
        done,
        query_weight,
        key_weight,
        value_weight,
        out_grad[0],
        image_ids[0],
        own_picks[1],
        (tracker[0], tracker_mixed[0], tracker_copy[0], grad_prev[0]),
    )
    lower, upper, total = gossip(kept, part)
    tracker_mixed_new = (
        tracker_mixed[0].astype(jnp.float32)
        + mix_stream([lower, kept, upper], row_picks, 1, model_width)
    ).astype(jnp.bfloat16)
    entries = float(blk_count * model_width * model_width)
    return (
        weights_new[None],
        copies_new[None],
        mixed_new[None],
        tracker_new[None],
        tracker_copy_new[None],
        tracker_mixed_new[None],
        grad_new[None],
        total[0, 0] / entries,
    )


def solution(mesh):
    field = P("blk", None, "tp")
    return jax.shard_map(
        device_step,
        mesh=mesh,
        in_specs=(field,) * 7
        + (P("blk", "tp", None), P("blk", None), P(None, "tp"), P(None, "tp"), field, P()),
        out_specs=(field,) * 7 + (P(),),
        check_vma=False,
    )
```
